32 devices in a mesh: rows: 8 (over y, x, core), grp: 4 (over z).
Axes of the slice: x: 2, y: 2, z: 4, core: 2. Of those that a mesh axis runs over, the one named last changes fastest.
Arguments:
- matrix: bfloat16 [24576, 16384], P(('rows', 'grp')), may hold values from -3000 to 3000, as said below
- keep_mask: int32 [16, 24576], P(None, ('rows', 'grp')), may hold values 0 or 1
Outputs:
- cosine: float32 [16384, 256], P(('rows', 'grp'))
The draws below stay inside these ranges and needn't reach their ends.
Inputs may be any that keep to these rules, and one draw needn't show every extreme that they name: `matrix`: entries are real-valued; row and column magnitudes vary.
All inputs are finite; a program needn't handle non-finite values. No bound on the sum of `keep_mask` on one device may be relied on, other than what follows from the above.
Results may differ from the reference program's by a relative error of at most 0.0003.
Values sent between devices are 32-bit elements; how exact they have to be, the bound alone decides.
A program may use at most 192 MiB of HBM per device.

```python
import math
import jax
import jax.numpy as jnp
from jax import lax

COLS = 16384
BLOCK = 1024
WINDOW = 256
ROW_DEV = 768
NBLK = 16
ROWS_ALL = 24576


def draw_matrix(key, part):
    key_base, key_row, key_col = jax.random.split(jax.random.fold_in(key, 7), 3)
    position = jnp.arange(ROWS_ALL, dtype=jnp.float32) / ROWS_ALL
    row_scale = jnp.exp(position * math.log(3.0) + jax.random.uniform(key_row, (ROWS_ALL,), jnp.float32, 0.0, math.log(10.0)))
    col_scale = jnp.exp(jax.random.uniform(key_col, (COLS,), jnp.float32, 0.0, math.log(10.0)))
    base = jnp.clip(jax.random.normal(key_base, (ROWS_ALL, COLS), jnp.float32), -6.0, 6.0)
    return (base * row_scale[:, None] * col_scale[None, :]).astype(jnp.bfloat16)


def with_ends(array, key, low, top_value):
    shape = array.shape
    place = [jax.random.randint(jax.random.fold_in(key, axis), (), 0, shape[axis]) for axis in range(len(shape))]
    array = array.at[tuple(place)].set(low)
    longest = shape.index(max(shape))
    place[longest] = (place[longest] + 1) % shape[longest]
    return array.at[tuple(place)].set(top_value)


def setup_inputs(seed: int = 0) -> dict:
    arg_keys = jax.random.split(jax.random.key(seed), 3)
    matrix = draw_matrix(jax.random.fold_in(arg_keys[2], 71), 0)
    keep_mask = with_ends((jax.random.randint(arg_keys[1], (NBLK, ROWS_ALL), 0, 2) < 1).astype(jnp.int32), jax.random.fold_in(arg_keys[1], 1), 0, 1)
    return {"matrix": matrix, "keep_mask": keep_mask}


def reference(matrix, keep_mask):
    steps_count = ROWS_ALL // ROW_DEV
    blocks = matrix.reshape(steps_count, ROW_DEV, COLS)
    masks = keep_mask.reshape(NBLK, steps_count, ROW_DEV).transpose(1, 0, 2)

    def accumulate(carry, item):
        square, raw = carry
        block, block_mask = item
        square = square + lax.optimization_barrier(jnp.sum(jnp.square(block.astype(jnp.float32)), axis=0))
        gate = block_mask.T.astype(jnp.bfloat16)
        masked = (block.reshape(ROW_DEV, NBLK, BLOCK) * gate[:, :, None]).reshape(ROW_DEV, COLS)
        raw = raw + jnp.dot(masked.T, masked[:, :WINDOW], preferred_element_type=jnp.float32)
        return ((square, raw), None)
    start = (jnp.zeros((COLS,), jnp.float32), jnp.zeros((COLS, WINDOW), jnp.float32))
    (square, raw), _ = lax.scan(accumulate, start, (blocks, masks))
    inverse = 1.0 / jnp.sqrt(square + 1e-06)
    return raw * inverse[:, None] * inverse[None, :WINDOW]
```

```python
import contextlib
import functools

import jax
import jax.numpy as jnp
from jax import lax
from jax.experimental import pallas as pl
from jax.experimental.pallas import tpu as pltpu
from jax.sharding import PartitionSpec as P

WINDOW = 256
LANES = 128
STAT = 8
SUB = 256
SLOTS = 4
STAGES = 4
RESTS = 8
MESH = pl.DeviceIdType.MESH
KINDS = {"A": "xyz", "B": "yxz", "C": "zxy", "D": "zyx", "E": "xzy", "F": "yzx"}
HEIGHTS = (
    ("A0", 24),
    ("B0", 24),
    ("C0", 16),
    ("D0", 8),
    ("E0", 16),
    ("F0", 16),
    ("A1", 16),
    ("A2", 16),
    ("A3", 16),
    ("B1", 24),
    ("B2", 16),
    ("B3", 16),
    ("C1", 8),
    ("E1", 24),
    ("F1", 16),
)
EARLY = ("A0", "B0", "C0", "D0", "E0", "F0")
STAT_KIND = "A"
LIMIT = 50
ORDER = (
    ("R", "R", 0),
    ("Z", "C0", 1),
    ("R", "R", 1),
    ("R", "R", 2),
    ("F", "A0", 0),
    ("F", "B0", 0),
    ("R", "R", 3),
    ("R", "R", 4),
    ("R", "R", 5),
    ("R", "R", 6),
    ("R", "R", 7),
    ("S", "E1", 0),
    ("S", "A1", 0),
    ("S", "T", 0),
    ("S", "F1", 0),
    ("Z", "C1", 0),
    ("S", "B1", 0),
    ("S", "A2", 0),
    ("S", "B2", 0),
    ("F", "E0", 0),
    ("Z", "E0", 0),
    ("Z", "E0", 1),
    ("Z", "E0", 2),
    ("F", "F0", 0),
    ("Z", "F0", 0),
    ("Z", "C1", 1),
    ("Z", "C1", 2),
    ("Z", "D0", 1),
    ("F", "B0", 1),
    ("Z", "B0", 0),
    ("Z", "B0", 1),
    ("F", "E1", 0),
    ("Z", "E1", 0),
    ("Z", "E1", 1),
    ("F", "B1", 0),
    ("S", "A3", 0),
    ("Z", "C0", 2),
    ("F", "A0", 1),
    ("Z", "A0", 0),
    ("Z", "F0", 1),
    ("S", "B3", 0),
    ("F", "F1", 0),
    ("Z", "F1", 0),
    ("Z", "B0", 2),
    ("Z", "A0", 1),
    ("F", "B2", 0),
    ("F", "A2", 0),
    ("Z", "D0", 2),
    ("F", "A1", 0),
    ("F", "T", 0),
    ("Z", "F1", 1),
    ("Z", "A0", 2),
    ("Z", "F0", 2),
    ("F", "B1", 1),
    ("Z", "B1", 0),
    ("Z", "B1", 1),
    ("F", "B3", 0),
    ("F", "A2", 1),
    ("Z", "A2", 0),
    ("F", "A3", 0),
    ("Z", "F1", 2),
    ("Z", "C0", 3),
    ("F", "A1", 1),
    ("F", "T", 1),
    ("Z", "A1", 0),
    ("Z", "T", 0),
    ("Z", "A1", 1),
    ("Z", "T", 1),
    ("F", "B2", 1),
    ("Z", "B2", 0),
    ("Z", "D0", 3),
    ("Z", "C1", 3),
    ("Z", "A2", 1),
    ("F", "A3", 1),
    ("Z", "A3", 0),
    ("F", "B3", 1),
    ("Z", "B3", 0),
    ("Z", "E1", 2),
    ("Z", "E1", 3),
    ("Z", "E0", 3),
    ("Z", "B1", 2),
    ("Z", "B1", 3),
    ("Z", "F0", 3),
    ("Z", "B2", 1),
    ("Z", "F1", 3),
    ("Z", "A0", 3),
    ("F", "C1", 1),
    ("Z", "A3", 1),
    ("F", "D0", 1),
    ("Z", "A2", 2),
    ("Z", "A2", 3),
    ("F", "C0", 1),
    ("Z", "B0", 3),
    ("F", "E1", 2),
    ("Z", "A1", 2),
    ("Z", "T", 2),
    ("Z", "B2", 2),
    ("Z", "B2", 3),
    ("F", "F0", 2),
    ("F", "F1", 2),
    ("Z", "B3", 1),
    ("F", "E0", 2),
    ("Z", "A1", 3),
    ("Z", "T", 3),
    ("Z", "A3", 2),
    ("Z", "A3", 3),
    ("Z", "B3", 2),
    ("F", "C0", 2),
    ("F", "C1", 2),
    ("F", "D0", 2),
    ("Z", "B3", 3),
)


def scope(name):
    return contextlib.nullcontext()


class Piece:
    def __init__(self, name, start, height, order, stat):
        self.name, self.start, self.height = name, start, height
        self.order, self.stat, self.kind = order, stat, name[0]


def pieces():
    out, at = {}, 0
    for name, height in HEIGHTS:
        out[name] = Piece(name, at, height, KINDS[name[0]], False)
        at += height
    assert at == WINDOW
    out["T"] = Piece("T", 0, STAT, KINDS[STAT_KIND], True)
    return out


def groups_of(sizes, order, phase):
    fixed = order[:phase]
    return [
        (dx, dy)
        for dx in reversed(range(sizes["x"]))
        for dy in reversed(range(sizes["y"]))
        if not ("x" in fixed and dx) and not ("y" in fixed and dy)
    ]


def exchange(sizes, order, phase):
    axis = order[phase]
    i = "xy".index(axis)
    kept = [g for g in groups_of(sizes, order, phase) if g[i] == 0]
    sent = [
        [(d, g[1]) if axis == "x" else (g[0], d) for g in kept]
        for d in range(1, sizes[axis])
    ]
    return kept, sent


def buffers(sizes, tile):
    out = []
    for p in pieces().values():
        unit = LANES if p.stat else tile
        for phase, axis in enumerate(p.order):
            if axis == "z":
                n = len(groups_of(sizes, p.order, phase))
                for way in ("up", "down"):
                    shape = (max(1, sizes["z"] - 1), n, p.height, unit)
                    out.append(((p.name, way), shape))
            else:
                kept, sent = exchange(sizes, p.order, phase)
                cols = unit if "z" in p.order[:phase] else sizes["z"] * unit
                shape = (max(1, len(sent)), len(kept), p.height, cols)
                out.append(((p.name, phase), shape))
    return out


def semaphores(sizes):
    recv, send = {}, {}
    for p in pieces().values():
        for phase, axis in enumerate(p.order):
            send.setdefault((p.kind, phase), len(send))
            if axis == "z":
                for t in range(sizes["z"] - 1):
                    recv[p.name, "up", t + 1] = len(recv)
                    recv[p.name, "down", t] = len(recv)
            else:
                recv[p.name, phase] = len(recv)
    return recv, send


def kernel(cfg, matrix_ref, keep_hbm, out_ref, acc, stat, sib_out, sib_in, stat_out,
           stat_in, mbuf, keep_ref, panel, masked, load_sem, keep_sem, sib_send,
           sib_recv, send_sem, recv_sem, *bufs):
    X, Y, Z, tile, width, step = (
        cfg["x"], cfg["y"], cfg["z"], cfg["tile"], cfg["width"], cfg["step"]
    )
    span = Z * tile
    halves = span // step
    per = step // tile
    rows = lax.axis_index("rows")
    z = lax.axis_index("grp")
    c = lax.rem(rows, 2)
    x = lax.rem(rows // 2, X)
    y = rows // (2 * X)

    def device(yy, xx, cc, zz):
        return ((yy * X + xx) * 2 + cc, zz)

    def quad(g):
        return lax.rem(y + g[1], Y) * X + lax.rem(x + g[0], X)

    def peer(axis, d):
        if axis == "x":
            return device(y, lax.rem(x + d, X), c, z)
        return device(lax.rem(y + d, Y), x, c, z)

    peers = [device(y, x, 1 - c, z)]
    for axis, n in (("x", X), ("y", Y)):
        peers += [peer(axis, d) for d in range(1, n)]
    barrier = pltpu.get_barrier_semaphore()
    for p in peers:
        pl.semaphore_signal(barrier, inc=1, device_id=p, device_id_type=MESH)

    @pl.when(z > 0)
    def _():
        pl.semaphore_signal(
            barrier, inc=1, device_id=device(y, x, c, z - 1), device_id_type=MESH
        )

    @pl.when(z < Z - 1)
    def _():
        pl.semaphore_signal(
            barrier, inc=1, device_id=device(y, x, c, z + 1), device_id_type=MESH
        )

    def await_peers():
        n = len(peers) + jnp.where(z > 0, 1, 0) + jnp.where(z < Z - 1, 1, 0)
        pl.semaphore_wait(barrier, n)

    groups = [(dx, dy) for dx in reversed(range(X)) for dy in reversed(range(Y))]
    units = [(groups[0], h) for h in range(halves)]
    units += [(g, h) for h in range(halves) for g in groups[1:-1]]
    units += [(groups[-1], h) for h in range(halves)]
    steps = [(g, own, h) for g, h in units for own in (0, 1)]

    def base(s):
        g, own, h = s
        cc = c if own else 1 - c
        return pl.multiple_of((quad(g) * 2 + cc) * span + h * step, step)

    def load(i):
        return pltpu.make_async_copy(
            matrix_ref.at[:, pl.ds(base(steps[i]), step)],
            mbuf.at[i % SLOTS],
            load_sem.at[i % SLOTS],
        )

    window = pltpu.make_async_copy(
        matrix_ref.at[:, pl.ds(0, WINDOW)],
        mbuf.at[SLOTS - 1, :, pl.ds(0, WINDOW)],
        load_sem.at[SLOTS - 1],
    )
    keep = pltpu.make_async_copy(keep_hbm, keep_ref, keep_sem)
    window.start()
    keep.start()
    for i in range(SLOTS - 1):
        load(i).start()

    with scope("head"):
        window.wait()
        keep.wait()
        first = mbuf[SLOTS - 1, :, pl.ds(0, WINDOW)].astype(jnp.float32)
        window_sq = jnp.sum(first * first, axis=0, keepdims=True)
        panel[...] = first.T * keep_ref[pl.ds(0, 1), :].astype(jnp.float32)
    load(SLOTS - 1).start()
    lines = [window_sq[:, k : k + LANES] for k in range(0, WINDOW, LANES)]
    own_lines = tile // LANES
    blank = jnp.zeros((STAT - own_lines - len(lines), LANES), jnp.float32)

    def compute(i, dst, stat_dst):
        load(i).wait()
        block = base(steps[i]) // width
        gate = keep_ref[pl.ds(block, 1), :].astype(jnp.float32)
        masked[...] = (panel[...] * gate).astype(jnp.bfloat16)
        squares = []
        for j in range(step // SUB):
            piece = mbuf[i % SLOTS, :, pl.ds(j * SUB, SUB)]
            dst[:, pl.ds(j * SUB, SUB)] = jnp.dot(
                masked[...], piece, preferred_element_type=jnp.float32
            )
            wide = piece.astype(jnp.float32)
            sq = jnp.sum(wide * wide, axis=0, keepdims=True)
            squares += [sq[:, k : k + LANES] for k in range(0, SUB, LANES)]
        for t in range(per):
            mine = squares[t * own_lines : (t + 1) * own_lines]
            stat_dst[:, pl.ds(t * LANES, LANES)] = jnp.concatenate(
                mine + lines + [blank], axis=0
            )
        if i + SLOTS < len(steps):
            load(i + SLOTS).start()

    made = pieces()
    early = [made[n] for n in EARLY]
    first_rows = sum(p.height for p in early)
    ref_of = {key: ref for (key, _), ref in zip(buffers(cfg, tile), bufs)}
    incoming, outgoing = semaphores(cfg)
    twin = device(y, x, 1 - c, z)

    def awaited(ref, sem):
        return pltpu.make_async_remote_copy(
            src_ref=ref, dst_ref=ref, send_sem=sem, recv_sem=sem,
            device_id=twin, device_id_type=MESH,
        )

    def arrived(ref, sem):
        awaited(ref, sem).wait_recv()

    def sent_all(ref, sem):
        awaited(ref, sem).wait_send()

    def array(p):
        return (stat, LANES) if p.stat else (acc, tile)

    def z_copy(p, way, k, t, to):
        src, unit = array(p)
        phase = p.order.index("z")
        g = groups_of(cfg, p.order, phase)[k]
        return pltpu.make_async_remote_copy(
            src_ref=src.at[quad(g), pl.ds(p.start, p.height), pl.ds(t * unit, unit)],
            dst_ref=ref_of[p.name, way].at[t - 1 if way == "up" else t, k],
            send_sem=send_sem.at[outgoing[p.kind, phase]],
            recv_sem=recv_sem.at[incoming[p.name, way, t]],
            device_id=device(y, x, c, to),
            device_id_type=MESH,
        )

    def xy_copies(p, phase, only=None):
        src, unit = array(p)
        axis = p.order[phase]
        kept, sent = exchange(cfg, p.order, phase)
        out = []
        for d in range(len(sent)):
            for k, g in enumerate(sent[d]):
                if "z" in p.order[:phase]:
                    cols = [pl.ds(pl.multiple_of(z * unit, unit), unit)]
                elif phase == 0 and p in early:
                    part = Z * unit // halves
                    cols = [pl.ds(h * part, part) for h in range(halves)]
                else:
                    cols = [pl.ds(0, Z * unit)]
                for h, part in enumerate(cols):
                    if only is not None and only != (g, h):
                        continue
                    dst = ref_of[p.name, phase].at[d, k]
                    if len(cols) > 1:
                        dst = ref_of[p.name, phase].at[d, k, :, part]
                    out.append(
                        pltpu.make_async_remote_copy(
                            src_ref=src.at[quad(g), pl.ds(p.start, p.height), part],
                            dst_ref=dst,
                            send_sem=send_sem.at[outgoing[p.kind, phase]],
                            recv_sem=recv_sem.at[incoming[p.name, phase]],
                            device_id=peer(axis, d + 1),
                            device_id_type=MESH,
                        )
                    )
        return out

    def z_stage(p, s):
        src, unit = array(p)
        phase = p.order.index("z")
        here = groups_of(cfg, p.order, phase)

        def take(way, t):
            ref = ref_of[p.name, way].at[t - 1 if way == "up" else t]
            arrived(ref, recv_sem.at[incoming[p.name, way, t]])
            for k, g in enumerate(here):
                where = (quad(g), pl.ds(p.start, p.height), pl.ds(t * unit, unit))
                src[where] += ref[k]

        @pl.when(z == s)
        def _():
            for t in reversed(range(s, Z)):
                if s > 0:
                    take("up", t)
                if t > s:
                    for k in range(len(here)):
                        z_copy(p, "up", k, t, s + 1).start()

        top = Z - 1 - s

        @pl.when(z == top)
        def _():
            for t in range(top + 1):
                if s > 0:
                    take("down", t)
                if t < top:
                    for k in range(len(here)):
                        z_copy(p, "down", k, t, top - 1).start()

    def begin(p, phase):
        if phase < len(p.order) and p.order[phase] != "z":
            for copy in xy_copies(p, phase):
                copy.start()

    def finish(p, phase):
        src, unit = array(p)
        kept, sent = exchange(cfg, p.order, phase)
        if not sent:
            return
        ref = ref_of[p.name, phase]
        arrived(ref, recv_sem.at[incoming[p.name, phase]])
        if "z" in p.order[:phase]:
            cols = pl.ds(pl.multiple_of(z * unit, unit), unit)
        else:
            cols = pl.ds(0, Z * unit)
        for k, g in enumerate(kept):
            where = (quad(g), pl.ds(p.start, p.height), cols)
            total = src[where]
            for d in range(len(sent)):
                total = total + ref[d, k]
            src[where] = total

    cuts = ((0, first_rows), (first_rows, WINDOW - first_rows))

    def to_sibling(n, part):
        if part < 2:
            where = (n, pl.ds(*cuts[part]))
            src, dst = sib_out.at[where], sib_in.at[where]
            number = part * len(units) + n
        else:
            src, dst = stat_out.at[n], stat_in.at[n]
            number = 2 * len(units)
        pltpu.make_async_remote_copy(
            src_ref=src,
            dst_ref=dst,
            send_sem=sib_send.at[part],
            recv_sem=sib_recv.at[number],
            device_id=twin,
            device_id_type=MESH,
        ).start()

    def first_sends(p, g, h):
        if p.order[0] != "z":
            for copy in xy_copies(p, 0, (g, h)):
                copy.start()
            return
        k = groups_of(cfg, p.order, 0).index(g)
        tiles = range(h * per, (h + 1) * per)

        @pl.when(z == 0)
        def _():
            for t in reversed(tiles):
                if t > 0:
                    z_copy(p, "up", k, t, 1).start()

        @pl.when(z == Z - 1)
        def _():
            for t in tiles:
                if t < Z - 1:
                    z_copy(p, "down", k, t, Z - 2).start()

    def merge(n, part):
        g, h = units[n]
        q = quad(g)
        low, size = cuts[part]
        where = (n, pl.ds(low, size))
        arrived(sib_in.at[where], sib_recv.at[part * len(units) + n])

        def add(j, carry):
            at = pl.multiple_of(j * 8, 8)
            acc[q, pl.ds(at, 8), pl.ds(h * step, step)] += sib_in[n, pl.ds(at, 8), :]
            return carry

        lax.fori_loop(low // 8, (low + size) // 8, add, 0)
        if part == 0:
            for p in early:
                first_sends(p, g, h)

    def merge_stat():
        arrived(stat_in, sib_recv.at[2 * len(units)])
        for n, (g, h) in enumerate(units):
            stat[quad(g), :, pl.ds(h * per * LANES, per * LANES)] += stat_in[n]

    last = len(units) - 1
    for n, (g, h) in enumerate(units):
        with scope(f"a{n}"):
            compute(2 * n, sib_out.at[n], stat_out.at[n])
        if n == 0:
            with scope("barrier"):
                await_peers()
        to_sibling(n, 0)
        if n:
            to_sibling(n - 1, 1)
            to_sibling(n - 1, 2)
            with scope(f"m{n - 1}"):
                merge(n - 1, 0)
        with scope(f"b{n}"):
            compute(
                2 * n + 1,
                acc.at[quad(g), :, pl.ds(h * step, step)],
                stat.at[quad(g), :, pl.ds(h * per * LANES, per * LANES)],
            )
    to_sibling(last, 1)
    to_sibling(last, 2)
    with scope(f"m{last}"):
        merge(last, 0)

    def stages(s):
        return range(-(-s * Z // STAGES), -(-(s + 1) * Z // STAGES))

    def rest(n):
        return range(n * len(units) // RESTS, (n + 1) * len(units) // RESTS)

    for op in ORDER:
        if op[0] == "R":
            with scope(f"R{op[2]}"):
                for n in rest(op[2]):
                    merge(n, 1)
                    if n == last:
                        merge_stat()
            continue
        p = made[op[1]]
        if op[0] == "S":
            begin(p, 0)
        elif op[0] == "F":
            with scope(f"F{op[1]}.{op[2]}"):
                finish(p, op[2])
                begin(p, op[2] + 1)
        else:
            with scope(f"Z{op[1]}.{op[2]}"):
                for s in stages(op[2]):
                    if s > 0 or p not in early or p.order[0] != "z":
                        z_stage(p, s)
                if op[2] == STAGES - 1:
                    begin(p, p.order.index("z") + 1)

    with scope("final"):
        own = y * X + x
        tail = stat[own, :, pl.ds(pl.multiple_of(z * LANES, LANES), LANES)]
        tail = 1.0 / jnp.sqrt(tail + 1e-06)
        scale = jnp.concatenate([tail[k : k + 1] for k in range(own_lines)], axis=1)
        win = jnp.concatenate(
            [tail[own_lines + k : own_lines + k + 1] for k in range(len(lines))], axis=1
        )
        mine = acc[own, :, pl.ds(pl.multiple_of(z * tile, tile), tile)]
        out_ref[...] = (mine * scale).T * win

    with scope("drain"):
        for part in range(2):
            sent_all(sib_out.at[:, pl.ds(*cuts[part])], sib_send.at[part])
        sent_all(stat_out, sib_send.at[2])
        for (kind, phase), n in outgoing.items():
            same = [p for p in made.values() if p.kind == kind]
            src, unit = array(same[0])
            order = same[0].order
            if order[phase] == "z":
                count, cols = len(groups_of(cfg, order, phase)), (Z - 1) * unit
            else:
                kept, sent = exchange(cfg, order, phase)
                count = len(kept) * len(sent)
                cols = unit if "z" in order[:phase] else Z * unit
            high = sum(p.height for p in same)
            if count and cols:
                all_sent = src.at[pl.ds(0, count), pl.ds(0, high), pl.ds(0, cols)]
                sent_all(all_sent, send_sem.at[n])


def shards(matrix, keep_mask):
    depth, columns = matrix.shape
    blocks = keep_mask.shape[0]
    width = columns // blocks
    outer = lax.axis_size("rows")
    inner = lax.axis_size("grp")
    tile = columns // (outer * inner)
    span = inner * tile
    step = min(width, span)
    cfg = {"x": 2, "y": outer // 4, "z": inner, "tile": tile, "width": width}
    cfg["step"] = step
    quads = cfg["x"] * cfg["y"]
    links = quads * (span // step)
    recv, send = semaphores(cfg)
    flat = step // tile * LANES
    return pl.pallas_call(
        functools.partial(kernel, cfg),
        out_shape=jax.ShapeDtypeStruct((tile, WINDOW), jnp.float32),
        in_specs=[
            pl.BlockSpec(memory_space=pltpu.HBM),
            pl.BlockSpec(memory_space=pltpu.HBM),
        ],
        out_specs=pl.BlockSpec(memory_space=pltpu.VMEM),
        scratch_shapes=[
            pltpu.VMEM((quads, WINDOW, span), jnp.float32),
            pltpu.VMEM((quads, STAT, inner * LANES), jnp.float32),
            pltpu.VMEM((links, WINDOW, step), jnp.float32),
            pltpu.VMEM((links, WINDOW, step), jnp.float32),
            pltpu.VMEM((links, STAT, flat), jnp.float32),
            pltpu.VMEM((links, STAT, flat), jnp.float32),
            pltpu.VMEM((SLOTS, depth, step), jnp.bfloat16),
            pltpu.VMEM(keep_mask.shape, keep_mask.dtype),
            pltpu.VMEM((WINDOW, depth), jnp.float32),
            pltpu.VMEM((WINDOW, depth), jnp.bfloat16),
            pltpu.SemaphoreType.DMA((SLOTS,)),
            pltpu.SemaphoreType.DMA,
            pltpu.SemaphoreType.DMA((3,)),
            pltpu.SemaphoreType.DMA((2 * links + 1,)),
            pltpu.SemaphoreType.DMA((len(send),)),
            pltpu.SemaphoreType.DMA((len(recv),)),
        ]
        + [pltpu.VMEM(shape, jnp.float32) for _, shape in buffers(cfg, tile)],
        compiler_params=pltpu.CompilerParams(
            collective_id=0, has_side_effects=True, vmem_limit_bytes=LIMIT * 1024 * 1024
        ),
        cost_estimate=pl.CostEstimate(
            flops=2 * depth * columns * WINDOW,
            bytes_accessed=2 * depth * columns,
            transcendentals=0,
        ),
    )(matrix, pltpu.with_memory_space_constraint(keep_mask, pltpu.HBM))


def solution(mesh):
    in_specs = (P(("rows", "grp"), None), P(None, ("rows", "grp")))
    out_specs = P(("rows", "grp"), None)
    return jax.shard_map(
        shards, mesh=mesh, in_specs=in_specs, out_specs=out_specs, check_vma=False
    )
```

```python
import contextlib
import functools

import jax
import jax.numpy as jnp
from jax import lax
from jax.experimental import pallas as pl
from jax.experimental.pallas import tpu as pltpu
from jax.sharding import PartitionSpec as P

WINDOW = 256
LANES = 128
STAT = 8
SUB = 256
SLOTS = 4
MESH = pl.DeviceIdType.MESH
KINDS = {
    "A": "xypq", "B": "yxpq", "C": "pqxy", "D": "pqyx", "E": "xpyq", "F": "ypxq",
    "G": "pxyq", "H": "pyxq", "I": "pxqy", "J": "pyqx", "K": "xpqy", "L": "ypqx",
}
HEIGHTS = (
    ("E0", 16),
    ("D1", 8),
    ("B0", 32),
    ("B3", 16),
    ("C0", 16),
    ("D0", 16),
    ("C1", 16),
    ("A0", 40),
    ("B1", 24),
    ("A1", 16),
    ("B2", 16),
    ("A2", 16),
    ("B4", 8),
    ("A3", 8),
    ("B5", 8),
)
EARLY = ("E0", "D1", "B0", "B3", "C0", "D0", "C1", "A0", )
STAT_KIND = "F"
LIMIT = 50
ORDER = (
    ("R", "R", 0),
    ("S", "B1", 0),
    ("F", "B0", 0),
    ("F", "C0", 0),
    ("F", "E0", 0),
    ("F", "D0", 0),
    ("S", "A1", 0),
    ("F", "A0", 0),
    ("F", "B0", 1),
    ("F", "B1", 0),
    ("F", "C1", 0),
    ("S", "B2", 0),
    ("F", "A1", 0),
    ("F", "A0", 1),
    ("S", "A2", 0),
    ("S", "T", 0),
    ("F", "D1", 0),
    ("F", "B1", 1),
    ("F", "B2", 0),
    ("S", "B5", 0),
    ("F", "B0", 2),
    ("S", "B4", 0),
    ("F", "A1", 1),
    ("F", "B3", 0),
    ("F", "A2", 0),
    ("S", "A3", 0),
    ("F", "C1", 1),
    ("F", "T", 0),
    ("F", "E0", 1),
    ("F", "A0", 2),
    ("F", "B5", 0),
    ("F", "B2", 1),
    ("F", "B1", 2),
    ("F", "D1", 1),
    ("F", "C0", 1),
    ("F", "B3", 1),
    ("F", "A1", 2),
    ("F", "A3", 0),
    ("F", "B0", 3),
    ("F", "T", 1),
    ("F", "B4", 0),
    ("F", "A2", 1),
    ("F", "D0", 1),
    ("F", "C1", 2),
    ("F", "E0", 2),
    ("F", "B5", 1),
    ("F", "D1", 2),
    ("F", "B2", 2),
    ("F", "C0", 2),
    ("F", "A3", 1),
    ("F", "B3", 2),
    ("F", "D0", 2),
    ("F", "B4", 1),
    ("F", "A2", 2),
    ("F", "B5", 2),
    ("F", "T", 2),
    ("F", "B2", 3),
    ("F", "A3", 2),
    ("F", "B1", 3),
    ("F", "C0", 3),
    ("F", "A0", 3),
    ("F", "B4", 2),
    ("F", "D1", 3),
    ("F", "T", 3),
    ("F", "E0", 3),
    ("F", "A2", 3),
    ("F", "A3", 3),
    ("F", "C1", 3),
    ("F", "D0", 3),
    ("F", "B5", 3),
    ("F", "A1", 3),
    ("F", "B3", 3),
    ("F", "B4", 3),
)


def scope(name):
    return contextlib.nullcontext()


class Piece:
    def __init__(self, name, start, height, order, stat):
        self.name, self.start, self.height = name, start, height
        self.order, self.stat, self.kind = order, stat, name[0]


def bits_of(sizes):
    bits = sizes["z"].bit_length() - 1
    assert sizes["z"] == 1 << bits and bits <= 3
    return "pqr"[:bits]


def reversed_of(t, bits):
    return sum(((t >> k) & 1) << (bits - 1 - k) for k in range(bits))


def block_offsets(cfg):
    per, bits = cfg["step"] // cfg["tile"], len(bits_of(cfg))
    out = []
    for j in range(per):
        found = {
            reversed_of(low + j, bits) * cfg["tile"] // cfg["width"]
            for low in range(0, cfg["z"], per)
        }
        assert len(found) == 1
        out.append(found.pop())
    return out


def axes_of(sizes, kind):
    order = ""
    for axis in KINDS[kind]:
        order += axis
        if axis == "q":
            order += "r"
    return "".join(a for a in order if a in "xy" or a in bits_of(sizes))


def pieces(sizes):
    out, at = {}, 0
    for name, height in HEIGHTS:
        out[name] = Piece(name, at, height, axes_of(sizes, name[0]), False)
        at += height
    assert at == WINDOW
    out["T"] = Piece("T", 0, STAT, axes_of(sizes, STAT_KIND), True)
    return out


def held(sizes, order, phase):
    fixed = order[:phase]
    return [
        (dx, dy)
        for dx in reversed(range(sizes["x"]))
        for dy in reversed(range(sizes["y"]))
        if not ("x" in fixed and dx) and not ("y" in fixed and dy)
    ]


def exchange(sizes, order, phase):
    axis = order[phase]
    quads = held(sizes, order, phase)
    if axis not in "xy":
        return quads, [quads]
    i = "xy".index(axis)
    kept = [g for g in quads if g[i] == 0]
    sent = [
        [(d, g[1]) if axis == "x" else (g[0], d) for g in kept]
        for d in range(1, sizes[axis])
    ]
    return kept, sent


def slots_of(sizes, order, phase):
    done = sum(a not in "xy" for a in order[: phase + 1])
    return sizes["z"] >> done


def tiles_sent(sizes, order, phase):
    kept, sent = exchange(sizes, order, phase)
    return len(kept) * len(sent) * slots_of(sizes, order, phase)


def buffers(sizes, tile):
    out = []
    for p in pieces(sizes).values():
        unit = LANES if p.stat else tile
        for phase in range(len(p.order)):
            kept, sent = exchange(sizes, p.order, phase)
            cols = slots_of(sizes, p.order, phase) * unit
            shape = (max(1, len(sent)), len(kept), p.height, cols)
            out.append(((p.name, phase), shape))
    return out


def semaphores(sizes):
    recv, send = {}, {}
    for p in pieces(sizes).values():
        for phase in range(len(p.order)):
            send.setdefault((p.stat, tiles_sent(sizes, p.order, phase)), len(send))
            recv[p.name, phase] = len(recv)
    return recv, send


def kernel(cfg, matrix_ref, keep_hbm, out_ref, acc, stat, sib_out, sib_in, stat_out,
           stat_in, mbuf, keep_ref, panel, masked, load_sem, keep_sem, sib_send,
           sib_recv, send_sem, recv_sem, line_sem, *bufs):
    X, Y, Z, tile, width, step = (
        cfg["x"], cfg["y"], cfg["z"], cfg["tile"], cfg["width"], cfg["step"]
    )
    span = Z * tile
    halves = span // step
    per = step // tile
    rows = lax.axis_index("rows")
    z = lax.axis_index("grp")
    c = lax.rem(rows, 2)
    x = lax.rem(rows // 2, X)
    y = rows // (2 * X)

    def device(yy, xx, cc, zz):
        return ((yy * X + xx) * 2 + cc, zz)

    def quad(g):
        return lax.rem(y + g[1], Y) * X + lax.rem(x + g[0], X)

    def bit(axis):
        return lax.rem(z // (1 << "pqr".index(axis)), 2)

    def peer(axis, d):
        if axis == "x":
            return device(y, lax.rem(x + d, X), c, z)
        if axis == "y":
            return device(lax.rem(y + d, Y), x, c, z)
        return device(y, x, c, z + (1 << "pqr".index(axis)) * (1 - 2 * bit(axis)))

    short = Z <= 4
    peers = [device(y, x, 1 - c, z)]
    for axis, n in [("x", X), ("y", Y)] + [(b, 2) for b in bits_of(cfg) if not short]:
        peers += [peer(axis, d) for d in range(1, n)]
    below, above = jnp.where(z > 0, 1, 0), jnp.where(z < Z - 1, 1, 0)

    def tell(sem, device_id):
        pl.semaphore_signal(sem, inc=1, device_id=device_id, device_id_type=MESH)

    def tell_line(sem):
        @pl.when(z > 0)
        def _():
            tell(sem, device(y, x, c, z - 1))

        @pl.when(z < Z - 1)
        def _():
            tell(sem, device(y, x, c, z + 1))

    barrier = pltpu.get_barrier_semaphore()
    for p in peers:
        tell(barrier, p)
    if short:
        tell_line(barrier)

    def await_peers():
        pl.semaphore_wait(barrier, len(peers) + (below + above if short else 0))
        if short:
            tell_line(line_sem)

    names = bits_of(cfg)

    def reversed_bits(t):
        return reversed_of(t, len(names))

    groups = [(dx, dy) for dx in reversed(range(X)) for dy in reversed(range(Y))]
    units = [(groups[0], h) for h in range(halves)]
    units += [(g, h) for h in range(halves) for g in groups[1:-1]]
    units += [(groups[-1], h) for h in range(halves)]
    steps = [(g, own, h) for g, h in units for own in (0, 1)]

    def half(h):
        if halves != 2:
            return h
        return 1 - bit("p") if h == 0 else bit("p")

    def span_of(h, size):
        return pl.ds(pl.multiple_of(half(h) * size, size), size)

    def base(s):
        g, own, h = s
        cc = c if own else 1 - c
        return pl.multiple_of((quad(g) * 2 + cc) * span, span)

    def load(i):
        first, h = base(steps[i]), steps[i][2]
        for j in range(per):
            t = reversed_bits(half(h) * per + j)
            pltpu.make_async_copy(
                matrix_ref.at[:, pl.ds(pl.multiple_of(first + t * tile, tile), tile)],
                mbuf.at[i % SLOTS, :, pl.ds(j * tile, tile)],
                load_sem.at[i % SLOTS],
            ).start()

    def loaded(i):
        pltpu.make_async_copy(
            matrix_ref.at[:, pl.ds(0, step)], mbuf.at[i % SLOTS], load_sem.at[i % SLOTS]
        ).wait()

    window = pltpu.make_async_copy(
        matrix_ref.at[:, pl.ds(0, WINDOW)],
        mbuf.at[SLOTS - 1, :, pl.ds(0, WINDOW)],
        load_sem.at[SLOTS - 1],
    )
    keep = pltpu.make_async_copy(keep_hbm, keep_ref, keep_sem)
    window.start()
    keep.start()
    load(0)

    with scope("head"):
        window.wait()
        load(1)
        keep.wait()
        first = mbuf[SLOTS - 1, :, pl.ds(0, WINDOW)].astype(jnp.float32)
        window_sq = jnp.sum(first * first, axis=0, keepdims=True)
        panel[...] = first.T * keep_ref[pl.ds(0, 1), :].astype(jnp.float32)
    for i in range(2, SLOTS):
        load(i)
    lines = [window_sq[:, k : k + LANES] for k in range(0, WINDOW, LANES)]
    own_lines = tile // LANES
    blank = jnp.zeros((STAT - own_lines - len(lines), LANES), jnp.float32)

    offsets = block_offsets(cfg)
    kinds = sorted(set(offsets))

    def compute(i, dst, stat_dst):
        loaded(i)
        g, own, h = steps[i]
        at = (groups.index(g) * 2 + own) * len(kinds)
        if h == 0:
            for k, offset in enumerate(kinds):
                block = base(steps[i]) // width + offset
                gate = keep_ref[pl.ds(block, 1), :].astype(jnp.float32)
                masked[at + k] = (panel[...] * gate).astype(jnp.bfloat16)
        squares = []
        for j in range(step // SUB):
            piece = mbuf[i % SLOTS, :, pl.ds(j * SUB, SUB)]
            dst[:, pl.ds(j * SUB, SUB)] = jnp.dot(
                masked[at + kinds.index(offsets[j * SUB // tile])],
                piece,
                preferred_element_type=jnp.float32,
            )
            wide = piece.astype(jnp.float32)
            sq = jnp.sum(wide * wide, axis=0, keepdims=True)
            squares += [sq[:, k : k + LANES] for k in range(0, SUB, LANES)]
        for t in range(per):
            mine = squares[t * own_lines : (t + 1) * own_lines]
            stat_dst[:, pl.ds(t * LANES, LANES)] = jnp.concatenate(
                mine + lines + [blank], axis=0
            )
        if i + SLOTS < len(steps):
            load(i + SLOTS)

    made = pieces(cfg)
    early = [made[n] for n in EARLY]
    first_rows = sum(p.height for p in early)
    ref_of = {key: ref for (key, _), ref in zip(buffers(cfg, tile), bufs)}
    incoming, outgoing = semaphores(cfg)
    twin = device(y, x, 1 - c, z)

    def awaited(ref, sem):
        return pltpu.make_async_remote_copy(
            src_ref=ref, dst_ref=ref, send_sem=sem, recv_sem=sem,
            device_id=twin, device_id_type=MESH,
        )

    def arrived(ref, sem):
        awaited(ref, sem).wait_recv()

    def sent_all(ref, sem):
        awaited(ref, sem).wait_send()

    def array(p):
        return (stat, LANES) if p.stat else (acc, tile)

    def columns(p, phase, away):
        unit = array(p)[1]
        low = 0
        for axis in p.order[:phase]:
            if axis not in "xy":
                low += bit(axis) * (Z >> (names.index(axis) + 1))
        axis = p.order[phase]
        count = slots_of(cfg, p.order, phase)
        if axis not in "xy":
            low += (1 - bit(axis) if away else bit(axis)) * count
        if isinstance(low, int):
            return pl.ds(low * unit, count * unit)
        return pl.ds(pl.multiple_of(low * unit, unit), count * unit)

    def copy(p, phase, d, k, g, cols, part=None):
        src = array(p)[0]
        dst = ref_of[p.name, phase].at[d, k]
        if part is not None:
            dst = ref_of[p.name, phase].at[d, k, :, part]
        return pltpu.make_async_remote_copy(
            src_ref=src.at[quad(g), pl.ds(p.start, p.height), cols],
            dst_ref=dst,
            send_sem=send_sem.at[outgoing[p.stat, tiles_sent(cfg, p.order, phase)]],
            recv_sem=recv_sem.at[incoming[p.name, phase]],
            device_id=peer(p.order[phase], d + 1),
            device_id_type=MESH,
        )

    def begin(p, phase):
        if phase < len(p.order):
            cols = columns(p, phase, True)
            for d, quads in enumerate(exchange(cfg, p.order, phase)[1]):
                for k, g in enumerate(quads):
                    copy(p, phase, d, k, g, cols).start()

    def finish(p, phase):
        src = array(p)[0]
        kept, sent = exchange(cfg, p.order, phase)
        if not sent:
            return
        ref = ref_of[p.name, phase]
        arrived(ref, recv_sem.at[incoming[p.name, phase]])
        cols = columns(p, phase, False)
        for k, g in enumerate(kept):
            where = (quad(g), pl.ds(p.start, p.height), cols)
            total = src[where]
            for d in range(len(sent)):
                total = total + ref[d, k]
            src[where] = total

    links = []
    for p in early:
        links += [] if p.order[0] in [q.order[0] for q in links] else [p]
    head_rows = sum(p.height for p in links)
    ahead, behind, whole, later = (
        (0, head_rows),
        (head_rows, first_rows - head_rows),
        (0, first_rows),
        (first_rows, WINDOW - first_rows),
    )
    assert early[: len(links)] == links
    last = len(units) - 1

    def to_sibling(n, rows, number):
        if rows:
            where = (n, pl.ds(*rows))
            src, dst = sib_out.at[where], sib_in.at[where]
            kind = 1 if rows == later else 0
        else:
            src, dst, kind = stat_out.at[n], stat_in.at[n], 2
        pltpu.make_async_remote_copy(
            src_ref=src,
            dst_ref=dst,
            send_sem=sib_send.at[kind],
            recv_sem=sib_recv.at[number],
            device_id=twin,
            device_id_type=MESH,
        ).start()

    def offer(n):
        if n == 0 and behind[1]:
            to_sibling(0, ahead, 0)
            to_sibling(0, behind, last + 1)
        else:
            to_sibling(n, whole, n)

    def offer_rest(n):
        to_sibling(n, later, last + 2)
        to_sibling(n, None, last + 3)

    def first_sends(p, g, h):
        axis = p.order[0]
        for d, quads in enumerate(exchange(cfg, p.order, 0)[1]):
            if g not in quads:
                continue
            k = quads.index(g)
            if axis in "xy":
                part = span_of(h, step)
                copy(p, 0, d, k, g, part, part if halves > 1 else None).start()
            elif halves == 1:
                copy(p, 0, d, k, g, columns(p, 0, True)).start()
            elif halves == 2:
                if h == 0:
                    copy(p, 0, d, k, g, span_of(h, step)).start()
            else:

                @pl.when(bit(axis) == 1 - 2 * h // halves)
                def _():
                    part = pl.ds(h * step % (span // 2), step)
                    copy(p, 0, d, k, g, pl.ds(h * step, step), part).start()

    def add_rows(n, rows):
        g, h = units[n]
        q = quad(g)
        low, size = rows
        cols = span_of(h, step)

        def add(j, carry):
            at = pl.multiple_of(j * 8, 8)
            acc[q, pl.ds(at, 8), cols] += sib_in[n, pl.ds(at, 8), :]
            return carry

        lax.fori_loop(low // 8, (low + size) // 8, add, 0)
        for p in early:
            if low <= p.start < low + size:
                first_sends(p, g, h)

    def merge(n):
        parts = [(whole, n)]
        if n == 0 and behind[1]:
            parts = [(ahead, 0), (behind, last + 1)]
        for rows, number in parts:
            arrived(sib_in.at[n, pl.ds(*rows)], sib_recv.at[number])
            add_rows(n, rows)

    def merge_rest():
        arrived(sib_in.at[:, pl.ds(*later)], sib_recv.at[last + 2])
        for n in range(len(units)):
            add_rows(n, later)
        arrived(stat_in, sib_recv.at[last + 3])
        for n, (g, h) in enumerate(units):
            stat[quad(g), :, span_of(h, per * LANES)] += stat_in[n]

    for n, (g, h) in enumerate(units):
        with scope(f"a{n}"):
            compute(2 * n, sib_out.at[n], stat_out.at[n])
        if n == 0:
            with scope("barrier"):
                await_peers()
        offer(n)
        if n:
            offer_rest(n - 1)
        if n > 1:
            with scope(f"m{n - 1}"):
                merge(n - 1)
        with scope(f"b{n}"):
            compute(
                2 * n + 1,
                acc.at[quad(g), :, span_of(h, step)],
                stat.at[quad(g), :, span_of(h, per * LANES)],
            )
        if n == 0:
            with scope("m0"):
                merge(0)
    offer_rest(last)
    if last:
        with scope(f"m{last}"):
            merge(last)

    for op in ORDER:
        if op[0] == "R":
            if short:
                pl.semaphore_wait(line_sem, below + above)
            with scope("R"):
                merge_rest()
            continue
        p = made[op[1]]
        if op[0] == "S":
            begin(p, 0)
        elif op[2] < len(p.order):
            with scope(f"F{op[1]}.{op[2]}"):
                finish(p, op[2])
                begin(p, op[2] + 1)
    for p in made.values():
        for phase in range(4, len(p.order)):
            finish(p, phase)
            begin(p, phase + 1)

    with scope("final"):
        own = y * X + x
        slot = sum(bit(b) * (Z >> (k + 1)) for k, b in enumerate(names))
        tail = stat[own, :, pl.ds(pl.multiple_of(slot * LANES, LANES), LANES)]
        tail = 1.0 / jnp.sqrt(tail + 1e-06)
        scale = jnp.concatenate([tail[k : k + 1] for k in range(own_lines)], axis=1)
        win = jnp.concatenate(
            [tail[own_lines + k : own_lines + k + 1] for k in range(len(lines))], axis=1
        )
        mine = acc[own, :, pl.ds(pl.multiple_of(slot * tile, tile), tile)]
        out_ref[...] = (mine * scale).T * win

    with scope("drain"):
        sent_all(sib_out.at[:, pl.ds(*whole)], sib_send.at[0])
        sent_all(sib_out.at[:, pl.ds(*later)], sib_send.at[1])
        sent_all(stat_out, sib_send.at[2])
        for (is_stat, tiles), n in outgoing.items():
            high = sum(
                p.height
                for p in made.values()
                for phase in range(len(p.order))
                if p.stat == is_stat and tiles_sent(cfg, p.order, phase) == tiles
            )
            if tiles:
                src, unit = (stat, LANES) if is_stat else (acc, tile)
                wide = max(w for w in range(1, Z + 1) if tiles % w == 0)
                same = src.at[
                    pl.ds(0, tiles // wide), pl.ds(0, high), pl.ds(0, wide * unit)
                ]
                sent_all(same, send_sem.at[n])


def shards(matrix, keep_mask):
    depth, columns = matrix.shape
    blocks = keep_mask.shape[0]
    width = columns // blocks
    outer = lax.axis_size("rows")
    inner = lax.axis_size("grp")
    tile = columns // (outer * inner)
    span = inner * tile
    step = min(width, span)
    cfg = {"x": 2, "y": outer // 4, "z": inner, "tile": tile, "width": width}
    cfg["step"] = step
    quads = cfg["x"] * cfg["y"]
    links = quads * (span // step)
    recv, send = semaphores(cfg)
    flat = step // tile * LANES
    return pl.pallas_call(
        functools.partial(kernel, cfg),
        out_shape=jax.ShapeDtypeStruct((tile, WINDOW), jnp.float32),
        in_specs=[
            pl.BlockSpec(memory_space=pltpu.HBM),
            pl.BlockSpec(memory_space=pltpu.HBM),
        ],
        out_specs=pl.BlockSpec(memory_space=pltpu.VMEM),
        scratch_shapes=[
            pltpu.VMEM((quads, WINDOW, span), jnp.float32),
            pltpu.VMEM((quads, STAT, inner * LANES), jnp.float32),
            pltpu.VMEM((links, WINDOW, step), jnp.float32),
            pltpu.VMEM((links, WINDOW, step), jnp.float32),
            pltpu.VMEM((links, STAT, flat), jnp.float32),
            pltpu.VMEM((links, STAT, flat), jnp.float32),
            pltpu.VMEM((SLOTS, depth, step), jnp.bfloat16),
            pltpu.VMEM(keep_mask.shape, keep_mask.dtype),
            pltpu.VMEM((WINDOW, depth), jnp.float32),
            pltpu.VMEM((2 * quads * len(set(block_offsets(cfg))), WINDOW, depth), jnp.bfloat16),
            pltpu.SemaphoreType.DMA((SLOTS,)),
            pltpu.SemaphoreType.DMA,
            pltpu.SemaphoreType.DMA((3,)),
            pltpu.SemaphoreType.DMA((links + 3,)),
            pltpu.SemaphoreType.DMA((len(send),)),
            pltpu.SemaphoreType.DMA((len(recv),)),
            pltpu.SemaphoreType.REGULAR,
        ]
        + [pltpu.VMEM(shape, jnp.float32) for _, shape in buffers(cfg, tile)],
        compiler_params=pltpu.CompilerParams(
            collective_id=0, has_side_effects=True, vmem_limit_bytes=LIMIT * 1024 * 1024
        ),
        cost_estimate=pl.CostEstimate(
            flops=2 * depth * columns * WINDOW,
            bytes_accessed=2 * depth * columns,
            transcendentals=0,
        ),
    )(matrix, pltpu.with_memory_space_constraint(keep_mask, pltpu.HBM))


def solution(mesh):
    in_specs = (P(("rows", "grp"), None), P(None, ("rows", "grp")))
    out_specs = P(("rows", "grp"), None)
    return jax.shard_map(
        shards, mesh=mesh, in_specs=in_specs, out_specs=out_specs, check_vma=False
    )
```

```python
import contextlib
import functools

import jax
import jax.numpy as jnp
from jax import lax
from jax.experimental import pallas as pl
from jax.experimental.pallas import tpu as pltpu
from jax.sharding import PartitionSpec as P

WINDOW = 256
LANES = 128
STAT = 8
SUB = 256
SLOTS = 4
PHASES = 4
MESH = pl.DeviceIdType.MESH
KINDS = {
    "A": "xypq", "B": "yxpq", "C": "pqxy", "D": "pqyx", "E": "xpyq", "F": "ypxq",
    "G": "pxyq", "H": "pyxq", "I": "pxqy", "J": "pyqx", "K": "xpqy", "L": "ypqx",
}
HEIGHTS = (
    ("C0", 16),
    ("B3", 8),
    ("E0", 16),
    ("D1", 16),
    ("B0", 40),
    ("D0", 16),
    ("A1", 32),
    ("A0", 16),
    ("B1", 32),
    ("E1", 16),
    ("B2", 16),
    ("B4", 8),
    ("B5", 8),
    ("A2", 16),
)
EARLY = ("C0", "B3", "E0", "D1", "B0", "D0", "A1", )
STAT_KIND = "E"
LIMIT = 50
ORDER = (
    ("R", "R", 0),
    ("F", "C0", 0),
    ("S", "B1", 0),
    ("F", "B0", 0),
    ("G", "B0", 0),
    ("F", "A1", 0),
    ("F", "E0", 0),
    ("S", "A0", 0),
    ("F", "D0", 0),
    ("F", "B0", 1),
    ("F", "D1", 0),
    ("G", "A1", 0),
    ("S", "A2", 0),
    ("F", "A1", 1),
    ("F", "A0", 0),
    ("F", "B1", 0),
    ("G", "B0", 1),
    ("F", "B0", 2),
    ("G", "A0", 0),
    ("F", "A2", 0),
    ("G", "E0", 0),
    ("G", "A2", 0),
    ("F", "E0", 1),
    ("F", "A0", 1),
    ("G", "E0", 1),
    ("S", "B2", 0),
    ("G", "A0", 1),
    ("S", "B5", 0),
    ("G", "A1", 1),
    ("F", "A1", 2),
    ("G", "B1", 0),
    ("G", "C0", 0),
    ("F", "A2", 1),
    ("S", "E1", 0),
    ("F", "E0", 2),
    ("F", "B1", 1),
    ("F", "B3", 0),
    ("G", "B1", 1),
    ("G", "D0", 0),
    ("S", "T", 0),
    ("F", "E1", 0),
    ("S", "B4", 0),
    ("F", "B1", 2),
    ("G", "B3", 0),
    ("F", "B2", 0),
    ("G", "A1", 2),
    ("G", "E1", 0),
    ("F", "B3", 1),
    ("F", "A0", 2),
    ("F", "T", 0),
    ("F", "E1", 1),
    ("G", "B2", 0),
    ("F", "D0", 1),
    ("G", "D1", 0),
    ("G", "D0", 1),
    ("F", "B5", 0),
    ("F", "B2", 1),
    ("G", "T", 0),
    ("G", "A2", 1),
    ("G", "B0", 2),
    ("G", "B5", 0),
    ("F", "A2", 2),
    ("F", "B0", 3),
    ("G", "E0", 2),
    ("G", "A2", 2),
    ("F", "A1", 3),
    ("F", "B4", 0),
    ("F", "C0", 1),
    ("G", "B4", 0),
    ("G", "E1", 1),
    ("F", "D1", 1),
    ("F", "B5", 1),
    ("G", "B2", 1),
    ("F", "E1", 2),
    ("F", "B4", 1),
    ("G", "B3", 1),
    ("F", "T", 1),
    ("F", "B2", 2),
    ("G", "T", 1),
    ("G", "C0", 1),
    ("F", "B3", 2),
    ("G", "D1", 1),
    ("F", "D0", 2),
    ("F", "C0", 2),
    ("G", "B5", 1),
    ("F", "D1", 2),
    ("G", "A0", 2),
    ("F", "E0", 3),
    ("G", "B2", 2),
    ("F", "A2", 3),
    ("F", "T", 2),
    ("G", "B4", 1),
    ("G", "B1", 2),
    ("F", "B5", 2),
    ("F", "B4", 2),
    ("G", "B5", 2),
    ("G", "T", 2),
    ("F", "B1", 3),
    ("F", "T", 3),
    ("F", "A0", 3),
    ("G", "E1", 2),
    ("G", "B4", 2),
    ("G", "D0", 2),
    ("F", "E1", 3),
    ("F", "D0", 3),
    ("G", "D1", 2),
    ("G", "B3", 2),
    ("G", "C0", 2),
    ("F", "B3", 3),
    ("F", "B5", 3),
    ("F", "C0", 3),
    ("F", "B2", 3),
    ("F", "D1", 3),
    ("F", "B4", 3),
)


def scope(name):
    return contextlib.nullcontext()


class Piece:
    def __init__(self, name, start, height, order, stat):
        self.name, self.start, self.height = name, start, height
        self.order, self.stat, self.kind = order, stat, name[0]


def bits_of(sizes):
    bits = sizes["z"].bit_length() - 1
    assert sizes["z"] == 1 << bits and bits <= 3
    return "pqr"[:bits]


def reversed_of(t, bits):
    return sum(((t >> k) & 1) << (bits - 1 - k) for k in range(bits))


def block_offsets(cfg):
    per, bits = cfg["step"] // cfg["tile"], len(bits_of(cfg))
    out = []
    for j in range(per):
        found = {
            reversed_of(low + j, bits) * cfg["tile"] // cfg["width"]
            for low in range(0, cfg["z"], per)
        }
        assert len(found) == 1
        out.append(found.pop())
    return out


def axes_of(sizes, kind):
    order = ""
    for axis in KINDS[kind]:
        order += axis
        if axis == "q":
            order += "r"
    return "".join(a for a in order if a in "xy" or a in bits_of(sizes))


def pieces(sizes):
    out, at = {}, 0
    for name, height in HEIGHTS:
        out[name] = Piece(name, at, height, axes_of(sizes, name[0]), False)
        at += height
    assert at == WINDOW
    out["T"] = Piece("T", 0, STAT, axes_of(sizes, STAT_KIND), True)
    return out


def held(sizes, order, phase):
    fixed = order[:phase]
    return [
        (dx, dy)
        for dx in reversed(range(sizes["x"]))
        for dy in reversed(range(sizes["y"]))
        if not ("x" in fixed and dx) and not ("y" in fixed and dy)
    ]


def exchange(sizes, order, phase):
    axis = order[phase]
    quads = held(sizes, order, phase)
    if axis not in "xy":
        return quads, [quads]
    i = "xy".index(axis)
    kept = [g for g in quads if g[i] == 0]
    sent = [
        [(d, g[1]) if axis == "x" else (g[0], d) for g in kept]
        for d in range(1, sizes[axis])
    ]
    return kept, sent


def slots_of(sizes, order, phase):
    done = sum(a not in "xy" for a in order[: phase + 1])
    return sizes["z"] >> done


def parts_of(order, phase):
    return 2 if phase + 1 < len(order) else 1


def tiles_sent(sizes, order, phase):
    kept, sent = exchange(sizes, order, phase)
    return len(kept) * len(sent) * slots_of(sizes, order, phase)


def buffers(sizes, tile):
    out = []
    for p in pieces(sizes).values():
        unit = LANES if p.stat else tile
        for phase in range(len(p.order)):
            kept, sent = exchange(sizes, p.order, phase)
            cols = slots_of(sizes, p.order, phase) * unit
            shape = (max(1, len(sent)), len(kept), p.height, cols)
            out.append(((p.name, phase), shape))
    return out


def semaphores(sizes):
    recv, send = {}, {}
    for p in pieces(sizes).values():
        for phase in range(len(p.order)):
            send.setdefault((p.stat, tiles_sent(sizes, p.order, phase)), len(send))
            for part in range(parts_of(p.order, phase)):
                recv[p.name, phase, part] = len(recv)
    return recv, send


def kernel(cfg, matrix_ref, keep_hbm, out_ref, acc, stat, sib_out, sib_in, stat_out,
           stat_in, mbuf, keep_ref, panel, masked, load_sem, keep_sem, sib_send,
           sib_recv, send_sem, recv_sem, line_sem, *bufs):
    X, Y, Z, tile, width, step = (
        cfg["x"], cfg["y"], cfg["z"], cfg["tile"], cfg["width"], cfg["step"]
    )
    span = Z * tile
    halves = span // step
    assert halves <= 2
    per = step // tile
    rows = lax.axis_index("rows")
    z = lax.axis_index("grp")
    c = lax.rem(rows, 2)
    x = lax.rem(rows // 2, X)
    y = rows // (2 * X)

    def device(yy, xx, cc, zz):
        return ((yy * X + xx) * 2 + cc, zz)

    def quad(g):
        return lax.rem(y + g[1], Y) * X + lax.rem(x + g[0], X)

    def bit(axis):
        return lax.rem(z // (1 << "pqr".index(axis)), 2)

    def peer(axis, d):
        if axis == "x":
            return device(y, lax.rem(x + d, X), c, z)
        if axis == "y":
            return device(lax.rem(y + d, Y), x, c, z)
        return device(y, x, c, z + (1 << "pqr".index(axis)) * (1 - 2 * bit(axis)))

    short = Z <= 4
    peers = [device(y, x, 1 - c, z)]
    for axis, n in [("x", X), ("y", Y)] + [(b, 2) for b in bits_of(cfg) if not short]:
        peers += [peer(axis, d) for d in range(1, n)]
    below, above = jnp.where(z > 0, 1, 0), jnp.where(z < Z - 1, 1, 0)

    def tell(sem, device_id):
        pl.semaphore_signal(sem, inc=1, device_id=device_id, device_id_type=MESH)

    def tell_line(sem):
        @pl.when(z > 0)
        def _():
            tell(sem, device(y, x, c, z - 1))

        @pl.when(z < Z - 1)
        def _():
            tell(sem, device(y, x, c, z + 1))

    barrier = pltpu.get_barrier_semaphore()
    for p in peers:
        tell(barrier, p)
    if short:
        tell_line(barrier)

    def await_peers():
        pl.semaphore_wait(barrier, len(peers) + (below + above if short else 0))
        if short:
            tell_line(line_sem)

    names = bits_of(cfg)

    def reversed_bits(t):
        return reversed_of(t, len(names))

    groups = [(dx, dy) for dx in reversed(range(X)) for dy in reversed(range(Y))]
    units = [(groups[0], h) for h in range(halves)]
    units += [(g, h) for h in range(halves) for g in groups[1:-1]]
    units += [(groups[-1], h) for h in range(halves)]
    steps = [(g, own, h) for g, h in units for own in (0, 1)]

    def half(h):
        if halves != 2:
            return h
        return 1 - bit("p") if h == 0 else bit("p")

    def span_of(h, size):
        return pl.ds(pl.multiple_of(half(h) * size, size), size)

    def base(s):
        g, own, h = s
        cc = c if own else 1 - c
        return pl.multiple_of((quad(g) * 2 + cc) * span, span)

    def load(i):
        first, h = base(steps[i]), steps[i][2]
        for j in range(per):
            t = reversed_bits(half(h) * per + j)
            pltpu.make_async_copy(
                matrix_ref.at[:, pl.ds(pl.multiple_of(first + t * tile, tile), tile)],
                mbuf.at[i % SLOTS, :, pl.ds(j * tile, tile)],
                load_sem.at[i % SLOTS],
            ).start()

    def loaded(i):
        pltpu.make_async_copy(
            matrix_ref.at[:, pl.ds(0, step)], mbuf.at[i % SLOTS], load_sem.at[i % SLOTS]
        ).wait()

    window = pltpu.make_async_copy(
        matrix_ref.at[:, pl.ds(0, WINDOW)],
        mbuf.at[SLOTS - 1, :, pl.ds(0, WINDOW)],
        load_sem.at[SLOTS - 1],
    )
    keep = pltpu.make_async_copy(keep_hbm, keep_ref, keep_sem)
    window.start()
    keep.start()
    load(0)

    with scope("head"):
        window.wait()
        load(1)
        keep.wait()
        first = mbuf[SLOTS - 1, :, pl.ds(0, WINDOW)].astype(jnp.float32)
        window_sq = jnp.sum(first * first, axis=0, keepdims=True)
        panel[...] = first.T * keep_ref[pl.ds(0, 1), :].astype(jnp.float32)
    for i in range(2, SLOTS):
        load(i)
    lines = [window_sq[:, k : k + LANES] for k in range(0, WINDOW, LANES)]
    own_lines = tile // LANES
    blank = jnp.zeros((STAT - own_lines - len(lines), LANES), jnp.float32)

    offsets = block_offsets(cfg)
    kinds = sorted(set(offsets))

    def compute(i, dst, stat_dst):
        loaded(i)
        g, own, h = steps[i]
        at = (groups.index(g) * 2 + own) * len(kinds)
        if h == 0:
            for k, offset in enumerate(kinds):
                block = base(steps[i]) // width + offset
                gate = keep_ref[pl.ds(block, 1), :].astype(jnp.float32)
                masked[at + k] = (panel[...] * gate).astype(jnp.bfloat16)
        squares = []
        for j in range(step // SUB):
            piece = mbuf[i % SLOTS, :, pl.ds(j * SUB, SUB)]
            dst[:, pl.ds(j * SUB, SUB)] = jnp.dot(
                masked[at + kinds.index(offsets[j * SUB // tile])],
                piece,
                preferred_element_type=jnp.float32,
            )
            wide = piece.astype(jnp.float32)
            sq = jnp.sum(wide * wide, axis=0, keepdims=True)
            squares += [sq[:, k : k + LANES] for k in range(0, SUB, LANES)]
        for t in range(per):
            mine = squares[t * own_lines : (t + 1) * own_lines]
            stat_dst[:, pl.ds(t * LANES, LANES)] = jnp.concatenate(
                mine + lines + [blank], axis=0
            )
        if i + SLOTS < len(steps):
            load(i + SLOTS)

    made = pieces(cfg)
    early = [made[n] for n in EARLY]
    first_rows = sum(p.height for p in early)
    ref_of = {key: ref for (key, _), ref in zip(buffers(cfg, tile), bufs)}
    incoming, outgoing = semaphores(cfg)
    twin = device(y, x, 1 - c, z)

    def awaited(ref, sem):
        return pltpu.make_async_remote_copy(
            src_ref=ref, dst_ref=ref, send_sem=sem, recv_sem=sem,
            device_id=twin, device_id_type=MESH,
        )

    def arrived(ref, sem):
        awaited(ref, sem).wait_recv()

    def sent_all(ref, sem):
        awaited(ref, sem).wait_send()

    def array(p):
        return (stat, LANES) if p.stat else (acc, tile)

    def split(p, phase, part):
        kept = exchange(cfg, p.order, phase)[0]
        if phase + 1 == len(p.order):
            return list(range(len(kept))), None
        follow = p.order[phase + 1]
        if follow not in "xy":
            return list(range(len(kept))), follow
        i = "xy".index(follow)
        return [k for k, g in enumerate(kept) if (g[i] == 0) == (part == 1)], None

    def columns(p, phase, part, away):
        unit = array(p)[1]
        low = 0
        for axis in p.order[:phase]:
            if axis not in "xy":
                low += bit(axis) * (Z >> (names.index(axis) + 1))
        axis = p.order[phase]
        count = slots_of(cfg, p.order, phase)
        if axis not in "xy":
            low += (1 - bit(axis) if away else bit(axis)) * count
        inner, follow = 0, split(p, phase, part)[1]
        if follow:
            count //= 2
            inner = (bit(follow) if part else 1 - bit(follow)) * count

        def cut(at):
            if isinstance(at, int):
                return pl.ds(at * unit, count * unit)
            return pl.ds(pl.multiple_of(at * unit, unit), count * unit)

        return cut(low + inner), cut(inner)

    def copy(p, phase, part, d, k, g, cols, there):
        return pltpu.make_async_remote_copy(
            src_ref=array(p)[0].at[quad(g), pl.ds(p.start, p.height), cols],
            dst_ref=ref_of[p.name, phase].at[d, k, :, there],
            send_sem=send_sem.at[outgoing[p.stat, tiles_sent(cfg, p.order, phase)]],
            recv_sem=recv_sem.at[incoming[p.name, phase, part]],
            device_id=peer(p.order[phase], d + 1),
            device_id_type=MESH,
        )

    def begin(p, phase, only=None):
        if phase == len(p.order):
            return
        for part in range(parts_of(p.order, phase)):
            cols, there = columns(p, phase, part, True)
            for d, quads in enumerate(exchange(cfg, p.order, phase)[1]):
                for k in split(p, phase, part)[0]:
                    if only is None or quads[k] == only:
                        copy(p, phase, part, d, k, quads[k], cols, there).start()

    def finish(p, phase, part):
        src = array(p)[0]
        kept, sent = exchange(cfg, p.order, phase)
        touched = split(p, phase, part)[0]
        if not sent or not touched:
            return
        ref = ref_of[p.name, phase]
        cols, there = columns(p, phase, part, False)
        arrived(
            ref.at[:, pl.ds(0, len(touched)), :, pl.ds(0, cols.size)],
            recv_sem.at[incoming[p.name, phase, part]],
        )
        for k in touched:
            where = (quad(kept[k]), pl.ds(p.start, p.height), cols)
            total = src[where]
            for d in range(len(sent)):
                total = total + ref[d, k, :, there]
            src[where] = total

    links = []
    for p in early:
        links += [] if p.order[0] in [q.order[0] for q in links] else [p]
    head_rows = sum(p.height for p in links)
    ahead, behind, whole, later = (
        (0, head_rows),
        (head_rows, first_rows - head_rows),
        (0, first_rows),
        (first_rows, WINDOW - first_rows),
    )
    assert early[: len(links)] == links
    last = len(units) - 1

    def to_sibling(n, rows, number):
        if rows:
            where = (n, pl.ds(*rows))
            src, dst = sib_out.at[where], sib_in.at[where]
            kind = 1 if rows == later else 0
        else:
            src, dst, kind = stat_out.at[n], stat_in.at[n], 2
        pltpu.make_async_remote_copy(
            src_ref=src,
            dst_ref=dst,
            send_sem=sib_send.at[kind],
            recv_sem=sib_recv.at[number],
            device_id=twin,
            device_id_type=MESH,
        ).start()

    def offer(n):
        if n == 0 and behind[1]:
            to_sibling(0, ahead, 0)
            to_sibling(0, behind, last + 1)
        else:
            to_sibling(n, whole, n)

    def offer_rest(n):
        to_sibling(n, later, last + 2)
        to_sibling(n, None, last + 3)

    def first_sends(p, g, h):
        axis = p.order[0]
        if halves == 1 or axis not in "xy":
            if h == 0:
                begin(p, 0, g)
            return
        for part in range(2):
            touched, follow = split(p, 0, part)
            if follow and part != h:
                continue
            for d, quads in enumerate(exchange(cfg, p.order, 0)[1]):
                for k in touched:
                    if quads[k] == g:
                        cols = span_of(h, step)
                        copy(p, 0, part, d, k, g, cols, cols).start()

    def add_rows(n, rows):
        g, h = units[n]
        q = quad(g)
        low, size = rows
        cols = span_of(h, step)

        def add(j, carry):
            at = pl.multiple_of(j * 8, 8)
            acc[q, pl.ds(at, 8), cols] += sib_in[n, pl.ds(at, 8), :]
            return carry

        lax.fori_loop(low // 8, (low + size) // 8, add, 0)
        for p in early:
            if low <= p.start < low + size:
                first_sends(p, g, h)

    def merge(n):
        parts = [(whole, n)]
        if n == 0 and behind[1]:
            parts = [(ahead, 0), (behind, last + 1)]
        for rows, number in parts:
            arrived(sib_in.at[n, pl.ds(*rows)], sib_recv.at[number])
            add_rows(n, rows)

    def merge_rest():
        arrived(sib_in.at[:, pl.ds(*later)], sib_recv.at[last + 2])
        for n in range(len(units)):
            add_rows(n, later)
        arrived(stat_in, sib_recv.at[last + 3])
        for n, (g, h) in enumerate(units):
            stat[quad(g), :, span_of(h, per * LANES)] += stat_in[n]

    for n, (g, h) in enumerate(units):
        with scope(f"a{n}"):
            compute(2 * n, sib_out.at[n], stat_out.at[n])
        if n == 0:
            with scope("barrier"):
                await_peers()
        offer(n)
        if n:
            offer_rest(n - 1)
        if n > 1:
            with scope(f"m{n - 1}"):
                merge(n - 1)
        with scope(f"b{n}"):
            compute(
                2 * n + 1,
                acc.at[quad(g), :, span_of(h, step)],
                stat.at[quad(g), :, span_of(h, per * LANES)],
            )
        if n == 0:
            with scope("m0"):
                merge(0)
    offer_rest(last)
    if last:
        with scope(f"m{last}"):
            merge(last)

    for op in ORDER:
        if op[0] == "R":
            if short:
                pl.semaphore_wait(line_sem, below + above)
            with scope("R"):
                merge_rest()
            continue
        p = made[op[1]]
        if op[0] == "S":
            begin(p, 0)
        elif op[0] == "F":
            with scope(f"F{op[1]}.{op[2]}"):
                finish(p, op[2], 0)
                begin(p, op[2] + 1)
        else:
            with scope(f"G{op[1]}.{op[2]}"):
                finish(p, op[2], 1)
    for p in made.values():
        for phase in range(PHASES - 1, len(p.order)):
            if phase >= PHASES:
                finish(p, phase, 0)
                begin(p, phase + 1)
            if parts_of(p.order, phase) == 2:
                finish(p, phase, 1)

    with scope("final"):
        own = y * X + x
        slot = sum(bit(b) * (Z >> (k + 1)) for k, b in enumerate(names))
        tail = stat[own, :, pl.ds(pl.multiple_of(slot * LANES, LANES), LANES)]
        tail = 1.0 / jnp.sqrt(tail + 1e-06)
        scale = jnp.concatenate([tail[k : k + 1] for k in range(own_lines)], axis=1)
        win = jnp.concatenate(
            [tail[own_lines + k : own_lines + k + 1] for k in range(len(lines))], axis=1
        )
        mine = acc[own, :, pl.ds(pl.multiple_of(slot * tile, tile), tile)]
        out_ref[...] = (mine * scale).T * win

    with scope("drain"):
        sent_all(sib_out.at[:, pl.ds(*whole)], sib_send.at[0])
        sent_all(sib_out.at[:, pl.ds(*later)], sib_send.at[1])
        sent_all(stat_out, sib_send.at[2])
        for (is_stat, tiles), n in outgoing.items():
            high = sum(
                p.height
                for p in made.values()
                for phase in range(len(p.order))
                if p.stat == is_stat and tiles_sent(cfg, p.order, phase) == tiles
            )
            if tiles:
                src, unit = (stat, LANES) if is_stat else (acc, tile)
                wide = max(w for w in range(1, Z + 1) if tiles % w == 0)
                same = src.at[
                    pl.ds(0, tiles // wide), pl.ds(0, high), pl.ds(0, wide * unit)
                ]
                sent_all(same, send_sem.at[n])


def shards(matrix, keep_mask):
    depth, columns = matrix.shape
    blocks = keep_mask.shape[0]
    width = columns // blocks
    outer = lax.axis_size("rows")
    inner = lax.axis_size("grp")
    tile = columns // (outer * inner)
    span = inner * tile
    step = min(width, span)
    cfg = {"x": 2, "y": outer // 4, "z": inner, "tile": tile, "width": width}
    cfg["step"] = step
    quads = cfg["x"] * cfg["y"]
    links = quads * (span // step)
    recv, send = semaphores(cfg)
    flat = step // tile * LANES
    return pl.pallas_call(
        functools.partial(kernel, cfg),
        out_shape=jax.ShapeDtypeStruct((tile, WINDOW), jnp.float32),
        in_specs=[
            pl.BlockSpec(memory_space=pltpu.HBM),
            pl.BlockSpec(memory_space=pltpu.HBM),
        ],
        out_specs=pl.BlockSpec(memory_space=pltpu.VMEM),
        scratch_shapes=[
            pltpu.VMEM((quads, WINDOW, span), jnp.float32),
            pltpu.VMEM((quads, STAT, inner * LANES), jnp.float32),
            pltpu.VMEM((links, WINDOW, step), jnp.float32),
            pltpu.VMEM((links, WINDOW, step), jnp.float32),
            pltpu.VMEM((links, STAT, flat), jnp.float32),
            pltpu.VMEM((links, STAT, flat), jnp.float32),
            pltpu.VMEM((SLOTS, depth, step), jnp.bfloat16),
            pltpu.VMEM(keep_mask.shape, keep_mask.dtype),
            pltpu.VMEM((WINDOW, depth), jnp.float32),
            pltpu.VMEM((2 * quads * len(set(block_offsets(cfg))), WINDOW, depth), jnp.bfloat16),
            pltpu.SemaphoreType.DMA((SLOTS,)),
            pltpu.SemaphoreType.DMA,
            pltpu.SemaphoreType.DMA((3,)),
            pltpu.SemaphoreType.DMA((links + 3,)),
            pltpu.SemaphoreType.DMA((len(send),)),
            pltpu.SemaphoreType.DMA((len(recv),)),
            pltpu.SemaphoreType.REGULAR,
        ]
        + [pltpu.VMEM(shape, jnp.float32) for _, shape in buffers(cfg, tile)],
        compiler_params=pltpu.CompilerParams(
            collective_id=0, has_side_effects=True, vmem_limit_bytes=LIMIT * 1024 * 1024
        ),
        cost_estimate=pl.CostEstimate(
            flops=2 * depth * columns * WINDOW,
            bytes_accessed=2 * depth * columns,
            transcendentals=0,
        ),
    )(matrix, pltpu.with_memory_space_constraint(keep_mask, pltpu.HBM))


def solution(mesh):
    in_specs = (P(("rows", "grp"), None), P(None, ("rows", "grp")))
    out_specs = P(("rows", "grp"), None)
    return jax.shard_map(
        shards, mesh=mesh, in_specs=in_specs, out_specs=out_specs, check_vma=False
    )
```
